32 devices in a mesh: tm: 4 (over y, x), rows: 8 (over z, core).
Axes of the slice: x: 2, y: 2, z: 4, core: 2. Of those that a mesh axis runs over, the one named last changes fastest.
Arguments:
- frames_in: bfloat16 [16, 128, 64, 128], P('tm', 'rows'), may hold values from -6 to 6
- conv_one: bfloat16 [64, 3, 3, 64], replicated, may hold values from -0.375 to 0.375
- conv_two: bfloat16 [64, 3, 3, 64], replicated, may hold values from -0.375 to 0.375
- temporal: bfloat16 [3, 64, 64], replicated, may hold values from -0.625 to 0.625
- conv_three: bfloat16 [64, 3, 3, 64], replicated, may hold values from -0.375 to 0.375
- conv_four: bfloat16 [64, 3, 3, 64], replicated, may hold values from -0.375 to 0.375
- cotangent: bfloat16 [16, 128, 64, 128], P('tm', 'rows'), may hold values from -6 to 6
Outputs:
- decoded: bfloat16 [16, 128, 64, 128], P('tm', 'rows')
- grad_in: float32 [16, 128, 64, 128], P('tm', 'rows')
The draws below stay inside these ranges and needn't reach their ends.
All inputs are finite; a program needn't handle non-finite values.
Results may differ from the reference program's by a relative error of at most 0.013.
Values may be sent and summed in bfloat16 or wider, within the bound.
No kernel may reach another device: no remote copies, remote signals or barrier semaphores. Data moves between devices by JAX's collectives and lax.ppermute only.
A program may use at most 64 MiB of HBM per device.

```python
import jax
import jax.numpy as jnp
from jax import lax

C = 64
W = 128
FRAMES = 16
NROWS = 128


def level_of(stream_key, shape, shards, smallest, top_value):
    gain, own = 1.0, jax.random.fold_in(stream_key, 6)
    for axis_at, blocks in shards:
        heights = jnp.exp(jax.random.uniform(jax.random.fold_in(own, axis_at), (blocks,), jnp.float32, smallest / len(shards), top_value / len(shards)))
        gain = gain * jnp.repeat(heights, shape[axis_at] // blocks).reshape([-1 if axis == axis_at else 1 for axis in range(len(shape))])
    return gain


def gaussian(own_key, extent, deviation, reach, shards=(), held_as=jnp.bfloat16):
    drawn = deviation * jax.random.normal(own_key, extent, jnp.float32)
    if shards:
        drawn = drawn * level_of(own_key, extent, shards, -0.22, 0.18)
    return jnp.clip(drawn, -reach, reach).astype(held_as)


def setup_inputs(seed: int = 0) -> dict:
    key_list = jax.random.split(jax.random.key(seed), 8)
    return {
        "frames_in": gaussian(key_list[0], (FRAMES, NROWS, C, W), 1.0, 6.0, ((0, 4), (1, 8))),
        "conv_one": gaussian(key_list[1], (C, 3, 3, C), (9 * C // 2) ** -0.5, 0.375),
        "conv_two": gaussian(key_list[2], (C, 3, 3, C), (9 * C // 2) ** -0.5, 0.375),
        "temporal": gaussian(key_list[3], (3, C, C), (3 * C // 2) ** -0.5, 0.625),
        "conv_three": gaussian(key_list[4], (C, 3, 3, C), (9 * C // 2) ** -0.5, 0.375),
        "conv_four": gaussian(key_list[5], (C, 3, 3, C), (9 * C // 2) ** -0.5, 0.375),
        "cotangent": gaussian(key_list[6], (FRAMES, NROWS, C, W), 1.0, 6.0, ((0, 4), (1, 8))),
    }


SQRT_HALF = 0.7071067811865476
INV_ROOT_TAU = 0.3989422804014327


def gelu_value(v):
    return 0.5 * v * (1.0 + jax.scipy.special.erf(v * SQRT_HALF))


def gelu_slope(v):
    return 0.5 * (1.0 + jax.scipy.special.erf(v * SQRT_HALF)) + v * jnp.exp(-0.5 * v * v) * INV_ROOT_TAU


def flipped(kernel):
    return jnp.transpose(kernel[:, ::-1, ::-1, :], (3, 1, 2, 0))


def spatial(source, kernel):
    weights = kernel.reshape(kernel.shape[0], -1).astype(jnp.float32)
    padded = jnp.pad(source, ((0, 0), (1, 1), (0, 0), (1, 1)))
    row_count = source.shape[1]
    span_width = source.shape[3]

    def single(plane):
        columns = jnp.concatenate([plane[tap_row:tap_row + row_count, :, tap_col:tap_col + span_width]
                                   for tap_row in range(3) for tap_col in range(3)], axis=1).astype(jnp.float32)
        return jnp.einsum('ok,rkw->row', weights, columns, precision=lax.Precision.HIGHEST)

    return lax.map(single, padded)


def causal_mix(source, temporal):
    count = source.shape[0]
    padded = jnp.concatenate([jnp.zeros((2,) + source.shape[1:], source.dtype), source], axis=0).astype(jnp.float32)
    weights = temporal.astype(jnp.float32)
    total = jnp.zeros(source.shape, jnp.float32)
    for lag in range(3):
        total = total + jnp.einsum('oc,frcw->frow', weights[lag], padded[lag:lag + count], precision=lax.Precision.HIGHEST)
    return total


def causal_back(source, temporal):
    count = source.shape[0]
    padded = jnp.concatenate([source, jnp.zeros((2,) + source.shape[1:], source.dtype)], axis=0).astype(jnp.float32)
    weights = temporal.astype(jnp.float32)
    total = jnp.zeros(source.shape, jnp.float32)
    for lag in range(3):
        total = total + jnp.einsum('oc,frow->frcw', weights[lag], padded[2 - lag:2 - lag + count], precision=lax.Precision.HIGHEST)
    return total


def reference(frames_in, conv_one, conv_two, temporal, conv_three, conv_four, cotangent):
    pre_one = spatial(frames_in, conv_one)
    act_one = gelu_value(pre_one).astype(jnp.bfloat16)
    pre_two = spatial(act_one, conv_two)
    act_two = gelu_value(pre_two).astype(jnp.bfloat16)
    pre_three = causal_mix(act_two, temporal)
    act_three = gelu_value(pre_three).astype(jnp.bfloat16)
    pre_four = spatial(act_three, conv_three)
    act_four = gelu_value(pre_four).astype(jnp.bfloat16)
    decoded = spatial(act_four, conv_four).astype(jnp.bfloat16)
    back_four = (spatial(cotangent, flipped(conv_four)) * gelu_slope(pre_four)).astype(jnp.bfloat16)
    back_three = (spatial(back_four, flipped(conv_three)) * gelu_slope(pre_three)).astype(jnp.bfloat16)
    back_two = (causal_back(back_three, temporal) * gelu_slope(pre_two)).astype(jnp.bfloat16)
    back_one = (spatial(back_two, flipped(conv_two)) * gelu_slope(pre_one)).astype(jnp.bfloat16)
    grad_in = spatial(back_one, flipped(conv_one))
    return decoded, grad_in
```

```python
import functools

import jax
import jax.numpy as jnp
from jax import lax
from jax.experimental import pallas as pl
from jax.experimental.pallas import tpu as pltpu
from jax.sharding import PartitionSpec as P

SQRT_HALF = 0.7071067811865476
INV_ROOT_TAU = 0.3989422804014327
LOG2_E = 1.4426950408889634
BF16 = jnp.bfloat16
F32 = jnp.float32
VMEM = pl.BlockSpec(memory_space=pltpu.VMEM)
ANY = pl.BlockSpec(memory_space=pl.ANY)
WIDE = 4


def passed_along(value, axis, steps):
    count = lax.axis_size(axis)
    first, last = (max(0, -steps), min(count, count - steps))
    return lax.ppermute(value, axis, [(source, source + steps) for source in range(first, last)])


def call(body, ins, in_specs, outs, out_specs, scratch=(), aliases=None, flops=0, name=None):
    return pl.pallas_call(
        body,
        out_shape=outs,
        in_specs=in_specs,
        out_specs=out_specs,
        scratch_shapes=list(scratch),
        input_output_aliases=aliases or {},
        cost_estimate=pl.CostEstimate(flops=flops, transcendentals=0, bytes_accessed=1 << 20),
        compiler_params=pltpu.CompilerParams(vmem_limit_bytes=48 * 1024 * 1024),
        name=name,
    )(*ins)


def edge_masks():
    at, count = lax.axis_index("rows"), lax.axis_size("rows")
    return jnp.where(at > 0, 1.0, 0.0), jnp.where(at < count - 1, 1.0, 0.0)


def masked(value, row, halo, rows, masks):
    if row < halo:
        return value * masks[0]
    if row >= rows - halo:
        return value * masks[1]
    return value


def cdf_of(v):
    return 0.5 * lax.erf(v * SQRT_HALF) + 0.5


def slope_of(v, cdf):
    return cdf + v * jnp.exp2(v * v * (-0.5 * LOG2_E)) * INV_ROOT_TAU


def shifted(v):
    width = v.shape[-1]
    lane = lax.broadcasted_iota(jnp.int32, v.shape, v.ndim - 1)
    left = jnp.where(lane == 0, 0.0, pltpu.roll(v, 1, v.ndim - 1))
    right = jnp.where(lane == width - 1, 0.0, pltpu.roll(v, width - 1, v.ndim - 1))
    return left.astype(BF16), v.astype(BF16), right.astype(BF16)


def put(triple, f, r, v):
    for ref, part in zip(triple, shifted(v)):
        ref[f, r] = part


def window(ref, f, r):
    rows, chan, width = 4, ref.shape[-2], ref.shape[-1]
    return ref[f, r : r + rows].reshape(rows * chan, width)


def contract(weights, sources, tasks, finish):
    for at in range(0, len(tasks), WIDE):
        group = tasks[at : at + WIDE]
        rhs = jnp.concatenate(
            [jnp.concatenate([source(f, r) for f, r in group], axis=1) for source in sources], axis=0
        )
        total = jnp.dot(weights[...], rhs, preferred_element_type=F32)
        width = total.shape[1] // len(group)
        for j, (f, r) in enumerate(group):
            part = total[:, j * width : (j + 1) * width]
            finish(f, r, part.reshape(2, part.shape[0] // 2, width))


def conv(weights, triple, frames, rows, finish):
    tasks = [(f, r) for r in range(0, rows, 2) for f in frames]
    contract(weights, [functools.partial(window, ref) for ref in triple], tasks, finish)


def fill(triple, f, pieces):
    at = 0
    for ref, frame, first, rows in pieces:
        for r in range(rows):
            put(triple, f, at, ref[frame, first + r].astype(F32))
            at += 1


def toeplitz(blocks):
    zero = jnp.zeros_like(blocks[0])
    top = jnp.concatenate(list(blocks) + [zero], axis=1)
    bottom = jnp.concatenate([zero] + list(blocks), axis=1)
    return jnp.concatenate([top, bottom], axis=0).astype(BF16)


def prep_body(*refs):
    kernels, temporal = refs[:4], refs[4]
    forward, backward, mix, unmix = refs[5:]
    wide = 4 * temporal.shape[1]
    for n, ref in enumerate(kernels):
        whole = ref[...].astype(F32)
        for b in range(3):
            own = [whole[:, a, b, :] for a in range(3)]
            forward[n, :, b * wide : (b + 1) * wide] = toeplitz(own)
            back = [part.T for part in own[::-1]]
            backward[n, :, (2 - b) * wide : (3 - b) * wide] = toeplitz(back)
    lags = [temporal[j].astype(F32) for j in range(3)]
    mix[...] = toeplitz(lags)
    unmix[...] = toeplitz([lag.T for lag in lags[::-1]])


def pack_body(source, cot, last, first, sems):
    rows = source.shape[1]
    copies = [
        pltpu.make_async_copy(source.at[:, rows - 4 :], last.at[:, :4], sems.at[0]),
        pltpu.make_async_copy(cot.at[:, rows - 2 :], last.at[:, 4:], sems.at[1]),
        pltpu.make_async_copy(source.at[:, :4], first.at[:, :4], sems.at[2]),
        pltpu.make_async_copy(cot.at[:, :2], first.at[:, 4:], sems.at[3]),
    ]
    for copy in copies:
        copy.start()
    for copy in copies:
        copy.wait()


def encode_body(base, source, above, below, forward, act_two, slope_one, slope_two, *scratch):
    src, mid = scratch[:3], scratch[3:]
    masks = edge_masks()
    rows = source.shape[1]
    for f in range(2):
        fill(src, f, [(above, base + f, 0, 4), (source, base + f, 0, rows), (below, base + f, 0, 4)])

    def first(f, r, v):
        for i in range(2):
            x = v[i]
            cdf = cdf_of(x)
            put(mid, f, r + i, masked(x * cdf, r + i, 3, rows + 6, masks))
            if 2 <= r + i < rows + 4:
                slope_one[f, r + i - 2] = slope_of(x, cdf).astype(BF16)

    def second(f, r, v):
        for i in range(2):
            x = v[i]
            cdf = cdf_of(x)
            act_two[f, r + i] = masked(x * cdf, r + i, 2, rows + 4, masks).astype(BF16)
            if 2 <= r + i < rows + 2:
                slope_two[f, r + i - 2] = slope_of(x, cdf).astype(BF16)

    conv(forward.at[0], src, range(2), rows + 6, first)
    conv(forward.at[1], mid, range(2), rows + 4, second)


def emit(dst, base, buf, sems, frames, rows, step):
    def send(f, r):
        copy = pltpu.make_async_copy(
            buf.at[f, pl.ds(r, step)], dst.at[base + f, pl.ds(r, step)], sems.at[f, r // step]
        )
        copy.start()
        return copy

    return send


def decode_into(weights, triple, rows, buf, dst, base, sems):
    copies = []

    def finish(f, r, v):
        buf[f, r : r + 2] = v.astype(buf.dtype)
        if r % 4 == 2:
            copies.append(emit(dst, base, buf, sems, 2, rows, 4)(f, r - 2))

    conv(weights, triple, range(2), rows, finish)
    return copies


def middle_body(base, decode, *refs):
    refs = list(refs)
    early, late, cot, above, below, forward, backward, mix = refs[:8]
    refs = refs[8:]
    masks = edge_masks()
    rows = cot.shape[1]
    back_three, rest = refs[0], refs[1:]
    side, rest = rest[0], rest[1:]
    three, four, seed, back = rest[:3], rest[3:6], rest[6:9], rest[9:12]
    slope_three, slope_four = rest[12:14]

    def stack(f, r):
        return jnp.concatenate([early[0, r], early[1, r], late[0, r], late[1, r]], axis=0)

    def mixed(f, r, v):
        for i in range(2):
            x = v[i]
            cdf = cdf_of(x)
            put(three, i, r, x * cdf)
            if 2 <= r < rows + 2:
                slope_three[i, r - 2] = slope_of(x, cdf).astype(BF16)

    contract(mix, [stack], [(0, r) for r in range(rows + 4)], mixed)
    for f in range(2):
        fill(seed, f, [(above, base + f, 4, 2), (cot, base + f, 0, rows), (below, base + f, 4, 2)])

    def third(f, r, v):
        for i in range(2):
            x = v[i]
            cdf = cdf_of(x)
            act = masked(x * cdf, r + i, 1, rows + 2, masks)
            if decode:
                put(four, f, r + i, act)
            else:
                side[f, r + i] = act.astype(BF16)
            slope_four[f, r + i] = slope_of(x, cdf).astype(BF16)

    conv(forward.at[2], three, range(2), rows + 2, third)

    def fourth(f, r, v):
        for i in range(2):
            x = v[i] * slope_four[f, r + i].astype(F32)
            put(back, f, r + i, masked(x, r + i, 1, rows + 2, masks))

    conv(backward.at[3], seed, range(2), rows + 2, fourth)

    def fifth(f, r, v):
        for i in range(2):
            back_three[f, r + i] = (v[i] * slope_three[f, r + i].astype(F32)).astype(BF16)

    conv(backward.at[2], back, range(2), rows, fifth)
    if decode:
        buf, sems = rest[14:]
        for copy in decode_into(forward.at[3], four, rows, buf, side, base, sems):
            copy.wait()


def decode_body(base, act_four, forward, whole, out, *scratch):
    four, (buf, sems) = scratch[:3], scratch[3:]
    rows = act_four.shape[1] - 2
    for f in range(2):
        fill(four, f, [(act_four, f, 0, rows + 2)])
    for copy in decode_into(forward.at[3], four, rows, buf, out, base, sems):
        copy.wait()


def unmix_body(early, late, slope, unmix, back_two, last, first):
    rows = slope.shape[1]

    def stack(f, r):
        return jnp.concatenate([early[0, r], early[1, r], late[0, r], late[1, r]], axis=0)

    def finish(f, r, v):
        for i in range(2):
            value = (v[i] * slope[i, r].astype(F32)).astype(BF16)
            back_two[i, r] = value
            if r < 2:
                first[i, r] = value
            if r >= rows - 2:
                last[i, r - rows + 2] = value

    contract(unmix, [stack], [(0, r) for r in range(rows)], finish)


def grad_body(base, back_two, above, below, slope, backward, *refs):
    out, refs = refs[-9], refs[-8:]
    src, mid, (buf, sems) = refs[:3], refs[3:6], refs[6:]
    masks = edge_masks()
    rows = back_two.shape[1]
    for f in range(2):
        fill(src, f, [(above, f, 0, 2), (back_two, f, 0, rows), (below, f, 0, 2)])

    def first(f, r, v):
        for i in range(2):
            x = v[i] * slope[f, r + i].astype(F32)
            put(mid, f, r + i, masked(x, r + i, 1, rows + 2, masks))

    conv(backward.at[1], src, range(2), rows + 2, first)
    for copy in decode_into(backward.at[0], mid, rows, buf, out, base, sems):
        copy.wait()


def per_device(frames_in, conv_one, conv_two, temporal, conv_three, conv_four, cotangent):
    count, rows, chan, width = frames_in.shape
    unit = rows * chan * chan * width * 2 * 9 * 2

    def arr(*lead, dtype=BF16):
        return jax.ShapeDtypeStruct(tuple(lead) + (chan, width), dtype)

    def vm(*lead, dtype=BF16):
        return pltpu.VMEM(tuple(lead) + (chan, width), dtype)

    sems = pltpu.SemaphoreType.DMA((2, rows // 4))

    last, first = call(
        pack_body, (frames_in, cotangent), [ANY] * 2, [arr(count, 6)] * 2, [VMEM] * 2,
        [pltpu.SemaphoreType.DMA((4,))], name="pack",
    )
    above = passed_along(last, "rows", 1)
    below = passed_along(first, "rows", -1)
    two, four = 2 * chan, 4 * chan
    forward, backward, mix, unmix = call(
        prep_body, (conv_one, conv_two, conv_three, conv_four, temporal), [VMEM] * 5,
        [jax.ShapeDtypeStruct((4, two, 3 * four), BF16)] * 2
        + [jax.ShapeDtypeStruct((two, four), BF16)] * 2,
        [VMEM] * 4, flops=unit // 4, name="prep",
    )

    def encode(base):
        return call(
            functools.partial(encode_body, base), (frames_in, above, below, forward), [VMEM] * 4,
            [arr(2, rows + 4), arr(2, rows + 2), arr(2, rows)], [VMEM] * 3,
            [vm(2, rows + 8)] * 3 + [vm(2, rows + 6)] * 3, flops=3 * unit, name=f"encode{base}",
        )

    def middle(base, early, late, decode):
        side = arr(count, rows) if decode else arr(2, rows + 2)
        scratch = [vm(2, rows + 4)] * 3 + [vm(2, rows + 2)] * 3 + [vm(2, rows + 4)] * 3
        scratch += [vm(2, rows + 2)] * 3 + [vm(2, rows), vm(2, rows + 2)]
        if decode:
            scratch += [vm(2, rows), sems]
        return call(
            functools.partial(middle_body, base, decode),
            (early, late, cotangent, above, below, forward, backward, mix), [VMEM] * 8,
            [arr(2, rows), side], [VMEM, ANY if decode else VMEM], scratch,
            flops=5 * unit, name=f"middle{base}",
        )

    def unmixed(early, late, slope, name):
        return call(
            unmix_body, (early, late, slope, unmix), [VMEM] * 4,
            [arr(2, rows), arr(2, 2), arr(2, 2)], [VMEM] * 3, flops=unit // 3, name=name,
        )

    def grad(base, back_two, last, first, slope, whole):
        above, below = passed_along(last, "rows", 1), passed_along(first, "rows", -1)
        ins, specs = (back_two, above, below, slope, backward), [VMEM] * 5
        if whole is not None:
            ins, specs = ins + (whole,), specs + [ANY]
        return call(
            functools.partial(grad_body, base), ins, specs, arr(count, rows, dtype=F32), ANY,
            [vm(2, rows + 4)] * 3 + [vm(2, rows + 2)] * 3 + [vm(2, rows, dtype=F32), sems],
            {} if whole is None else {5: 0}, flops=2 * unit, name=f"grad{base}",
        )

    act_late, slope_one_late, slope_two_late = encode(2)
    act_before = passed_along(act_late, "tm", 1)
    act_early, slope_one_early, slope_two_early = encode(0)
    back_three_late, decoded = middle(2, act_early, act_late, True)
    back_three_early, act_four = middle(0, act_before, act_early, False)
    back_after = passed_along(back_three_early, "tm", -1)
    bt_early, last_early, first_early = unmixed(back_three_early, back_three_late, slope_two_early, "unmix0")
    decoded = call(
        functools.partial(decode_body, 0), (act_four, forward, decoded), [VMEM, VMEM, ANY],
        arr(count, rows), ANY, [vm(2, rows + 2)] * 3 + [vm(2, rows), sems], {2: 0},
        flops=unit, name="decode0",
    )
    grad_in = grad(0, bt_early, last_early, first_early, slope_one_early, None)
    bt_late, last_late, first_late = unmixed(back_three_late, back_after, slope_two_late, "unmix2")
    grad_in = grad(2, bt_late, last_late, first_late, slope_one_late, grad_in)
    return decoded, grad_in


def solution(mesh):
    split = P("tm", "rows", None, None)
    return jax.shard_map(
        per_device,
        mesh=mesh,
        in_specs=(split, P(), P(), P(), P(), P(), split),
        out_specs=(split, split),
        check_vma=False,
    )
```

```python
import functools

import jax
import jax.numpy as jnp
from jax import lax
from jax.experimental import pallas as pl
from jax.experimental.pallas import tpu as pltpu
from jax.sharding import PartitionSpec as P

SQRT_HALF = 0.7071067811865476
INV_ROOT_TAU = 0.3989422804014327
LOG2_E = 1.4426950408889634
BF16 = jnp.bfloat16
F32 = jnp.float32
VMEM = pl.BlockSpec(memory_space=pltpu.VMEM)
ANY = pl.BlockSpec(memory_space=pl.ANY)
HBM = pl.BlockSpec(memory_space=pltpu.HBM)
WIDE = 4


def passed_along(value, axis, steps):
    count = lax.axis_size(axis)
    return lax.ppermute(value, axis, [(source, (source + steps) % count) for source in range(count)])


def call(body, ins, in_specs, outs, out_specs, scratch=(), aliases=None, flops=0, name=None):
    return pl.pallas_call(
        body,
        out_shape=outs,
        in_specs=in_specs,
        out_specs=out_specs,
        scratch_shapes=list(scratch),
        input_output_aliases=aliases or {},
        cost_estimate=pl.CostEstimate(flops=flops, transcendentals=0, bytes_accessed=1 << 20),
        compiler_params=pltpu.CompilerParams(vmem_limit_bytes=48 * 1024 * 1024),
        name=name,
    )(*ins)


def edge_masks(axis="rows"):
    at, count = lax.axis_index(axis), lax.axis_size(axis)
    return jnp.where(at > 0, 1.0, 0.0), jnp.where(at < count - 1, 1.0, 0.0)


def tied(value, *others):
    return lax.optimization_barrier((value,) + others)[0]


def masked(value, row, halo, rows, masks):
    if row < halo:
        return value * masks[0]
    if row >= rows - halo:
        return value * masks[1]
    return value


def cdf_of(v):
    return 0.5 * lax.erf(v * SQRT_HALF) + 0.5


def slope_of(v, cdf):
    return cdf + v * jnp.exp2(v * v * (-0.5 * LOG2_E)) * INV_ROOT_TAU


def shifted(v):
    width = v.shape[-1]
    lane = lax.broadcasted_iota(jnp.int32, v.shape, v.ndim - 1)
    left = jnp.where(lane == 0, 0.0, pltpu.roll(v, 1, v.ndim - 1))
    right = jnp.where(lane == width - 1, 0.0, pltpu.roll(v, width - 1, v.ndim - 1))
    return left.astype(BF16), v.astype(BF16), right.astype(BF16)


def put(triple, f, r, v):
    for ref, part in zip(triple, shifted(v)):
        ref[f, r] = part


def window(ref, f, r):
    rows, chan, width = 4, ref.shape[-2], ref.shape[-1]
    return ref[f, r : r + rows].reshape(rows * chan, width)


def contract(weights, sources, tasks, finish):
    for at in range(0, len(tasks), WIDE):
        group = tasks[at : at + WIDE]
        rhs = jnp.concatenate(
            [jnp.concatenate([source(f, r) for f, r in group], axis=1) for source in sources], axis=0
        )
        total = jnp.dot(weights[...], rhs, preferred_element_type=F32)
        width = total.shape[1] // len(group)
        for j, (f, r) in enumerate(group):
            part = total[:, j * width : (j + 1) * width]
            finish(f, r, part.reshape(2, part.shape[0] // 2, width))


def conv(weights, triple, frames, rows, finish):
    tasks = [(f, r) for r in range(0, rows, 2) for f in range(frames)]
    contract(weights, [functools.partial(window, ref) for ref in triple], tasks, finish)


def fill(triple, f, pieces):
    at = 0
    for ref, frame, rows, mask in pieces:
        for r in range(rows):
            v = ref[frame, r].astype(F32)
            put(triple, f, at, v if mask is None else v * mask)
            at += 1


def toeplitz(blocks):
    zero = jnp.zeros_like(blocks[0])
    top = jnp.concatenate(list(blocks) + [zero], axis=1)
    bottom = jnp.concatenate([zero] + list(blocks), axis=1)
    return jnp.concatenate([top, bottom], axis=0).astype(BF16)


def prep_body(*refs):
    kernels, temporal = refs[:4], refs[4]
    forward, backward, mix, unmix = refs[5:]
    wide = 4 * temporal.shape[1]
    for n, ref in enumerate(kernels):
        whole = ref[...].astype(F32)
        for b in range(3):
            own = [whole[:, a, b, :] for a in range(3)]
            forward[n, :, b * wide : (b + 1) * wide] = toeplitz(own)
            back = [part.T for part in own[::-1]]
            backward[n, :, (2 - b) * wide : (3 - b) * wide] = toeplitz(back)
    lags = [temporal[j].astype(F32) for j in range(3)]
    mix[...] = toeplitz(lags)
    unmix[...] = toeplitz([lag.T for lag in lags[::-1]])


def pack_body(source, cot, *refs):
    sems, rows, copies = refs[-1], source.shape[1], []
    for n, (whole, edge) in enumerate(((source, 4), (cot, 2))):
        for m, at in enumerate((rows - edge, 0)):
            part = whole.at[:, pl.ds(at, edge)]
            copies.append(pltpu.make_async_copy(part, refs[2 * n + m], sems.at[2 * n + m]))
    for copy in copies:
        copy.start()
    for copy in copies:
        copy.wait()


def encode_body(base, source, above, below, forward, act_two, slope_one, slope_two, *scratch):
    src, mid = scratch[:3], scratch[3:]
    masks = edge_masks()
    frames, rows = act_two.shape[0], source.shape[1]
    for f in range(frames):
        g = base + f
        fill(src, f, [(above, g, 4, masks[0]), (source, g, rows, None), (below, g, 4, masks[1])])

    def first(f, r, v):
        for i in range(2):
            x = v[i]
            cdf = cdf_of(x)
            put(mid, f, r + i, masked(x * cdf, r + i, 3, rows + 6, masks))
            if 2 <= r + i < rows + 4:
                slope_one[f, r + i - 2] = slope_of(x, cdf).astype(BF16)

    def second(f, r, v):
        for i in range(2):
            x = v[i]
            cdf = cdf_of(x)
            act_two[f, r + i] = masked(x * cdf, r + i, 2, rows + 4, masks).astype(BF16)
            if 2 <= r + i < rows + 2:
                slope_two[f, r + i - 2] = slope_of(x, cdf).astype(BF16)

    conv(forward.at[0], src, frames, rows + 6, first)
    conv(forward.at[1], mid, frames, rows + 4, second)


def decode_into(weights, triple, frames, rows, buf, dst, base, sems):
    copies = []

    def finish(f, r, v):
        buf[f, r : r + 2] = v.astype(buf.dtype)
        if r % 4 == 2:
            at = pl.ds(r - 2, 4)
            copies.append(pltpu.make_async_copy(buf.at[f, at], dst.at[base + f, at], sems.at[f, r // 4]))
            copies[-1].start()

    conv(weights, triple, frames, rows, finish)
    return copies


def middle_body(base, outside, decode, spots, *refs):
    acts, refs = list(zip(refs, spots)), refs[len(spots) :]
    cot, above, below, forward, backward, mix = refs[:6]
    back_three, side = refs[6:8]
    three, four, seed, back = refs[8:11], refs[11:14], refs[14:17], refs[17:20]
    slope_three, slope_four = refs[20:22]
    masks = edge_masks()
    frames, rows, chan = back_three.shape[0], cot.shape[1], cot.shape[2]
    weights = mix[: frames * chan, : len(acts) * chan]
    if outside:
        known = edge_masks("tm")[0]
        cut = outside * chan
        begin = (weights[:, :cut].astype(F32) * known).astype(BF16)
        weights = jnp.concatenate([begin, weights[:, cut:]], axis=1)

    def stack(r):
        return jnp.concatenate([ref[f, r] for ref, f in acts], axis=0)

    for at in range(0, rows + 4, WIDE):
        rhs = jnp.concatenate([stack(at + j) for j in range(WIDE)], axis=1)
        total = jnp.dot(weights, rhs, preferred_element_type=F32)
        width = total.shape[1] // WIDE
        for j in range(WIDE):
            r = at + j
            for i in range(frames):
                x = total[i * chan : (i + 1) * chan, j * width : (j + 1) * width]
                cdf = cdf_of(x)
                put(three, i, r, x * cdf)
                if 2 <= r < rows + 2:
                    slope_three[i, r - 2] = slope_of(x, cdf).astype(BF16)
    for f in range(frames):
        g = base + f
        fill(seed, f, [(above, g, 2, masks[0]), (cot, g, rows, None), (below, g, 2, masks[1])])

    def third(f, r, v):
        for i in range(2):
            x = v[i]
            cdf = cdf_of(x)
            act = masked(x * cdf, r + i, 1, rows + 2, masks)
            if decode:
                put(four, f, r + i, act)
            else:
                side[f, r + i] = act.astype(BF16)
            slope_four[f, r + i] = slope_of(x, cdf).astype(BF16)

    conv(forward.at[2], three, frames, rows + 2, third)

    def fourth(f, r, v):
        for i in range(2):
            x = v[i] * slope_four[f, r + i].astype(F32)
            put(back, f, r + i, masked(x, r + i, 1, rows + 2, masks))

    conv(backward.at[3], seed, frames, rows + 2, fourth)

    def fifth(f, r, v):
        for i in range(2):
            back_three[f, r + i] = (v[i] * slope_three[f, r + i].astype(F32)).astype(BF16)

    conv(backward.at[2], back, frames, rows, fifth)
    if decode:
        buf, sems = refs[22:]
        for copy in decode_into(forward.at[3], four, frames, rows, buf, side, base, sems):
            copy.wait()


def decode_body(base, one, two, forward, whole, out, *scratch):
    four, (buf, sems) = scratch[:3], scratch[3:]
    rows = one.shape[1] - 2
    for f, ref in enumerate((one, two)):
        fill(four, f, [(ref, 0, rows + 2, None)])
    for copy in decode_into(forward.at[3], four, 2, rows, buf, out, base, sems):
        copy.wait()


def unmix_body(outside, spots, *refs):
    picked = list(zip(refs, spots))
    backs, slopes = picked[:4], picked[4:]
    unmix, back_two, last, first = refs[6:]
    rows, chan = back_two.shape[1:3]
    weights = unmix[...]
    if outside:
        known = edge_masks("tm")[1]
        cut = (4 - outside) * chan
        end = (weights[:, cut:].astype(F32) * known).astype(BF16)
        weights = jnp.concatenate([weights[:, :cut], end], axis=1)
    for at in range(0, rows, WIDE):
        rhs = jnp.concatenate(
            [jnp.concatenate([ref[f, at + j] for ref, f in backs], axis=0) for j in range(WIDE)], axis=1
        )
        total = jnp.dot(weights, rhs, preferred_element_type=F32)
        width = total.shape[1] // WIDE
        for j in range(WIDE):
            r = at + j
            for i in range(2):
                x = total[i * chan : (i + 1) * chan, j * width : (j + 1) * width]
                slope, f = slopes[i]
                value = (x * slope[f, r].astype(F32)).astype(BF16)
                back_two[i, r] = value
                if r < 2:
                    first[i, r] = value
                if r >= rows - 2:
                    last[i, r - rows + 2] = value


def grad_body(base, spots, back_two, above, below, *refs):
    slopes, backward = list(zip(refs, spots)), refs[2]
    out, refs = refs[-9], refs[-8:]
    src, mid, (buf, sems) = refs[:3], refs[3:6], refs[6:]
    masks = edge_masks()
    frames, rows = back_two.shape[:2]
    for f in range(frames):
        fill(src, f, [(above, f, 2, masks[0]), (back_two, f, rows, None), (below, f, 2, masks[1])])

    def first(f, r, v):
        for i in range(2):
            slope, g = slopes[f]
            x = v[i] * slope[g, r + i].astype(F32)
            put(mid, f, r + i, masked(x, r + i, 1, rows + 2, masks))

    conv(backward.at[1], src, frames, rows + 2, first)
    for copy in decode_into(backward.at[0], mid, frames, rows, buf, out, base, sems):
        copy.wait()


def per_device(frames_in, conv_one, conv_two, temporal, conv_three, conv_four, cotangent):
    count, rows, chan, width = frames_in.shape
    unit = rows * chan * chan * width * 2 * 9 * 2

    def arr(*lead, dtype=BF16):
        return jax.ShapeDtypeStruct(tuple(lead) + (chan, width), dtype)

    def vm(*lead, dtype=BF16):
        return pltpu.VMEM(tuple(lead) + (chan, width), dtype)

    sems = pltpu.SemaphoreType.DMA((2, rows // 4))

    last, first, cot_last, cot_first = call(
        pack_body, (frames_in, cotangent), [HBM] * 2,
        [arr(count, 4)] * 2 + [arr(count, 2)] * 2, [VMEM] * 4,
        [pltpu.SemaphoreType.DMA((4,))], name="pack",
    )
    above = passed_along(last, "rows", 1)
    below = passed_along(first, "rows", -1)
    two, four = 2 * chan, 4 * chan
    forward, backward, mix, unmix = call(
        prep_body, (conv_one, conv_two, conv_three, conv_four, temporal), [VMEM] * 5,
        [jax.ShapeDtypeStruct((4, two, 3 * four), BF16)] * 2
        + [jax.ShapeDtypeStruct((two, four), BF16)] * 2,
        [VMEM] * 4, flops=unit // 4, name="prep",
    )

    def encode(base, n):
        return call(
            functools.partial(encode_body, base), (frames_in, above, below, forward), [VMEM] * 4,
            [arr(n, rows + 4), arr(n, rows + 2), arr(n, rows)], [VMEM] * 3,
            [vm(n, rows + 8)] * 3 + [vm(n, rows + 6)] * 3, flops=3 * unit * n // 2, name=f"encode{base}",
        )

    def middle(base, n, acts, outside):
        decode = len(acts) == 4
        acts, spots = zip(*acts)
        side = arr(count, rows) if decode else arr(n, rows + 2)
        scratch = [vm(n, rows + 4)] * 3 + [vm(n, rows + 2)] * 3 + [vm(n, rows + 4)] * 3
        scratch += [vm(n, rows + 2)] * 3 + [vm(n, rows), vm(n, rows + 2)]
        if decode:
            scratch += [vm(n, rows), sems]
        return call(
            functools.partial(middle_body, base, outside, decode, spots),
            acts + (cotangent, cot_above, cot_below, forward, backward, mix),
            [VMEM] * (len(acts) + 6), [arr(n, rows), side], [VMEM, ANY if decode else VMEM], scratch,
            flops=5 * unit * n // 2, name=f"middle{base}",
        )

    def unmixed(backs, slopes, outside, name):
        ins, spots = zip(*(backs + slopes))
        return call(
            functools.partial(unmix_body, outside, spots), ins + (unmix,), [VMEM] * 7,
            [arr(2, rows), arr(2, 2), arr(2, 2)], [VMEM] * 3, flops=unit // 3, name=name,
        )

    def grad(base, back_two, above, below, slopes, whole):
        slopes, spots = zip(*slopes)
        ins, specs = (back_two, above, below) + slopes + (backward,), [VMEM] * 6
        if whole is not None:
            ins, specs = ins + (whole,), specs + [ANY]
        return call(
            functools.partial(grad_body, base, spots), ins, specs, arr(count, rows, dtype=F32), ANY,
            [vm(2, rows + 4)] * 3 + [vm(2, rows + 2)] * 3 + [vm(2, rows, dtype=F32), sems],
            {} if whole is None else {6: 0}, flops=2 * unit, name=f"grad{base}",
        )

    act_3, slope_one_3, slope_two_3 = encode(3, 1)
    before_1 = passed_along(act_3, "tm", 1)
    act_2, slope_one_2, slope_two_2 = encode(2, 1)
    before_2 = passed_along(act_2, "tm", 1)
    cot_last, cot_first, act_2 = lax.optimization_barrier((cot_last, cot_first, act_2))
    cot_above = passed_along(cot_last, "rows", 1)
    cot_below = passed_along(cot_first, "rows", -1)
    act, slope_one, slope_two = encode(0, 2)
    back_1, act_four_1 = middle(1, 1, [(before_1, 0), (act, 0), (act, 1)], 1)
    after_1 = passed_along(back_1, "tm", -1)
    before_2, back_1 = lax.optimization_barrier((before_2, back_1))
    back_0, act_four_0 = middle(0, 1, [(before_2, 0), (before_1, 0), (act, 0)], 2)
    after_0 = passed_along(back_0, "tm", -1)
    act_3, back_0 = lax.optimization_barrier((act_3, back_0))
    back_late, decoded = middle(2, 2, [(act, 0), (act, 1), (act_2, 0), (act_3, 0)], 0)
    backs = [(back_0, 0), (back_1, 0), (back_late, 0), (back_late, 1), (after_0, 0), (after_1, 0)]
    early, last, first = unmixed(backs[:4], [(slope_two, 0), (slope_two, 1)], 0, "unmix0")
    early_above, early_below = passed_along(last, "rows", 1), passed_along(first, "rows", -1)
    late, last, first = unmixed(backs[2:], [(slope_two_2, 0), (slope_two_3, 0)], 2, "unmix2")
    late_above, late_below = passed_along(last, "rows", 1), passed_along(first, "rows", -1)
    decoded = call(
        functools.partial(decode_body, 0), (act_four_0, act_four_1, forward, decoded), [VMEM] * 3 + [ANY],
        arr(count, rows), ANY, [vm(2, rows + 2)] * 3 + [vm(2, rows), sems], {3: 0},
        flops=unit, name="decode0",
    )
    grad_in = grad(0, early, early_above, early_below, [(slope_one, 0), (slope_one, 1)], None)
    grad_in = grad(2, late, late_above, late_below, [(slope_one_2, 0), (slope_one_3, 0)], grad_in)
    return decoded, grad_in


def solution(mesh):
    split = P("tm", "rows", None, None)
    return jax.shard_map(
        per_device,
        mesh=mesh,
        in_specs=(split, P(), P(), P(), P(), P(), split),
        out_specs=(split, split),
        check_vma=False,
    )
```

```python
import functools

import jax
import jax.numpy as jnp
from jax import lax
from jax.experimental import pallas as pl
from jax.experimental.pallas import tpu as pltpu
from jax.sharding import PartitionSpec as P


SQRT_HALF = 0.7071067811865476
INV_ROOT_TAU = 0.3989422804014327
LOG2_E = 1.4426950408889634
BF16 = jnp.bfloat16
F32 = jnp.float32
VMEM = pl.BlockSpec(memory_space=pltpu.VMEM)
ANY = pl.BlockSpec(memory_space=pl.ANY)
HBM = pl.BlockSpec(memory_space=pltpu.HBM)
WIDE = 4


def passed_along(value, axis, steps):
    count = lax.axis_size(axis)
    return lax.ppermute(value, axis, [(source, (source + steps) % count) for source in range(count)])


def swapped(value, first):
    groups, count = lax.axis_size("tm"), lax.axis_size("rows")
    pairs = []
    for g in range(groups):
        aside = g ^ 1 if (g ^ 1) < groups else g
        for i in range(count):
            j = i + 1 if (i - first) % 2 == 0 else i - 1
            inside = 0 <= j < count
            pairs.append((g * count + i, g * count + j if inside else aside * count + i))
    return lax.ppermute(value, ("tm", "rows"), pairs)


def exchanged(near, far):
    return swapped(near, 0), swapped(far, 1)


def is_even():
    return lax.axis_index("rows") % 2 == 0


def call(body, ins, in_specs, outs, out_specs, scratch=(), aliases=None, flops=0, vmem=48):
    return pl.pallas_call(
        body,
        out_shape=outs,
        in_specs=in_specs,
        out_specs=out_specs,
        scratch_shapes=list(scratch),
        input_output_aliases=aliases or {},
        cost_estimate=pl.CostEstimate(flops=flops, transcendentals=0, bytes_accessed=1 << 20),
        compiler_params=pltpu.CompilerParams(vmem_limit_bytes=vmem * 1024 * 1024),
    )(*ins)


def edge_masks(axis="rows"):
    at, count = lax.axis_index(axis), lax.axis_size(axis)
    return jnp.where(at > 0, 1.0, 0.0), jnp.where(at < count - 1, 1.0, 0.0)


def masked(value, row, halo, rows, masks):
    if row < halo:
        return value * masks[0]
    if row >= rows - halo:
        return value * masks[1]
    return value


def cdf_of(v):
    return 0.5 * lax.erf(v * SQRT_HALF) + 0.5


def slope_of(v, cdf):
    return cdf + v * jnp.exp2(v * v * (-0.5 * LOG2_E)) * INV_ROOT_TAU


def shifted(v):
    width = v.shape[-1]
    lane = lax.broadcasted_iota(jnp.int32, v.shape, v.ndim - 1)
    left = jnp.where(lane == 0, 0.0, pltpu.roll(v, 1, v.ndim - 1))
    right = jnp.where(lane == width - 1, 0.0, pltpu.roll(v, width - 1, v.ndim - 1))
    return left.astype(BF16), v.astype(BF16), right.astype(BF16)


def put(triple, f, r, v):
    for ref, part in zip(triple, shifted(v)):
        ref[f, r] = part


def window(ref, f, r):
    rows, chan, width = 4, ref.shape[-2], ref.shape[-1]
    return ref[f, r : r + rows].reshape(rows * chan, width)


def contract(weights, sources, tasks, finish):
    for at in range(0, len(tasks), WIDE):
        group = tasks[at : at + WIDE]
        rhs = jnp.concatenate(
            [jnp.concatenate([source(f, r) for f, r in group], axis=1) for source in sources], axis=0
        )
        total = jnp.dot(weights[...], rhs, preferred_element_type=F32)
        width = total.shape[1] // len(group)
        for j, (f, r) in enumerate(group):
            part = total[:, j * width : (j + 1) * width]
            finish(f, r, part.reshape(2, part.shape[0] // 2, width))


def conv(weights, triple, frames, rows, finish):
    tasks = [(f, r) for r in range(0, rows, 2) for f in range(frames)]
    contract(weights, [functools.partial(window, ref) for ref in triple], tasks, finish)


def halos(near, far, at, rows, masks):
    even = is_even()

    def side(i, mask, first, second):
        return jnp.where(even, first[at + i].astype(F32), second[at + i].astype(F32)) * mask

    above = [functools.partial(side, i, masks[0], far, near) for i in range(rows)]
    below = [functools.partial(side, i, masks[1], near, far) for i in range(rows)]
    return above, below


def fill(triple, f, ref, g, rows, above=(), below=()):
    for i, row in enumerate(above):
        put(triple, f, i, row())
    for r in range(rows):
        put(triple, f, len(above) + r, ref[g, r].astype(F32))
    for i, row in enumerate(below):
        put(triple, f, len(above) + rows + i, row())


def toeplitz(blocks):
    zero = jnp.zeros_like(blocks[0])
    top = jnp.concatenate(list(blocks) + [zero], axis=1)
    bottom = jnp.concatenate([zero] + list(blocks), axis=1)
    return jnp.concatenate([top, bottom], axis=0).astype(BF16)


def prep_body(*refs):
    kernels, temporal = refs[:4], refs[4]
    forward, backward, mix, unmix = refs[5:]
    wide = 4 * temporal.shape[1]
    for n, ref in enumerate(kernels):
        for b in range(3):
            own = [ref[a, b].astype(F32) for a in range(3)]
            forward[n, :, b * wide : (b + 1) * wide] = toeplitz(own)
            back = [part.T for part in own[::-1]]
            backward[n, :, (2 - b) * wide : (3 - b) * wide] = toeplitz(back)
    lags = [temporal[j].astype(F32) for j in range(3)]
    mix[...] = toeplitz(lags)
    unmix[...] = toeplitz([lag.T for lag in lags[::-1]])


def take(whole, g, edge, near, far, at):
    last, even = whole.shape[1] - edge, is_even()
    near[at : at + edge] = whole[g, pl.ds(jnp.where(even, last, 0), edge)]
    far[at : at + edge] = whole[g, pl.ds(jnp.where(even, 0, last), edge)]


def pack_late_body(half, source, near, far):
    for g in range(half, source.shape[0]):
        take(source, g, 4, near, far, 4 * (g - half))


def pack_body(half, source, cot, near, far):
    for g in range(half):
        take(source, g, 4, near, far, 4 * g)
    for g in range(source.shape[0]):
        take(cot, g, 2, near, far, 4 * half + 2 * g)


def encode_body(base, at, source, near, far, forward, act_two, slope_one, slope_two, *scratch):
    src, mid = scratch[:3], scratch[3:]
    masks = edge_masks()
    frames, rows = act_two.shape[0], source.shape[1]
    for f in range(frames):
        fill(src, f, source, base + f, rows, *halos(near, far, at + 4 * f, 4, masks))

    def first(f, r, v):
        for i in range(2):
            x = v[i]
            cdf = cdf_of(x)
            put(mid, f, r + i, masked(x * cdf, r + i, 3, rows + 6, masks))
            if 2 <= r + i < rows + 4:
                slope_one[f, r + i - 2] = slope_of(x, cdf).astype(BF16)

    def second(f, r, v):
        for i in range(2):
            x = v[i]
            cdf = cdf_of(x)
            act_two[f, r + i] = masked(x * cdf, r + i, 2, rows + 4, masks).astype(BF16)
            if 2 <= r + i < rows + 2:
                slope_two[f, r + i - 2] = slope_of(x, cdf).astype(BF16)

    conv(forward.at[0], src, frames, rows + 6, first)
    conv(forward.at[1], mid, frames, rows + 4, second)


def decode_into(weights, triple, frames, rows, buf, dst, base, sems):
    copies = []

    def finish(f, r, v):
        buf[f, r : r + 2] = v.astype(buf.dtype)
        if r % 4 == 2:
            at = pl.ds(r - 2, 4)
            copies.append(pltpu.make_async_copy(buf.at[f, at], dst.at[base + f, at], sems.at[f, r // 4]))
            copies[-1].start()

    conv(weights, triple, frames, rows, finish)
    return copies


def middle_body(base, outside, decode, spots, *refs):
    acts, refs = list(zip(refs, spots)), refs[len(spots) :]
    cot, near, far, forward, backward, mix = refs[:6]
    back_three, side = refs[6:8]
    three, four, seed, back = refs[8:11], refs[11:14], refs[14:17], refs[17:20]
    slope_three, slope_four = refs[20:22]
    masks = edge_masks()
    frames, rows, chan = back_three.shape[0], cot.shape[1], cot.shape[2]
    weights = mix[: frames * chan, : len(acts) * chan]
    if outside:
        known = edge_masks("tm")[0]
        cut = outside * chan
        begin = (weights[:, :cut].astype(F32) * known).astype(BF16)
        weights = jnp.concatenate([begin, weights[:, cut:]], axis=1)

    def stack(r):
        return jnp.concatenate([ref[f, r] for ref, f in acts], axis=0)

    for at in range(0, rows + 4, WIDE):
        rhs = jnp.concatenate([stack(at + j) for j in range(WIDE)], axis=1)
        total = jnp.dot(weights, rhs, preferred_element_type=F32)
        width = total.shape[1] // WIDE
        for j in range(WIDE):
            r = at + j
            for i in range(frames):
                x = total[i * chan : (i + 1) * chan, j * width : (j + 1) * width]
                cdf = cdf_of(x)
                put(three, i, r, x * cdf)
                if 2 <= r < rows + 2:
                    slope_three[i, r - 2] = slope_of(x, cdf).astype(BF16)
    for f in range(frames):
        at = near.shape[0] - 2 * (cot.shape[0] - base - f)
        fill(seed, f, cot, base + f, rows, *halos(near, far, at, 2, masks))

    def third(f, r, v):
        for i in range(2):
            x = v[i]
            cdf = cdf_of(x)
            act = masked(x * cdf, r + i, 1, rows + 2, masks)
            if decode:
                put(four, f, r + i, act)
            else:
                side[f, r + i] = act.astype(BF16)
            slope_four[f, r + i] = slope_of(x, cdf).astype(BF16)

    conv(forward.at[2], three, frames, rows + 2, third)

    def fourth(f, r, v):
        for i in range(2):
            x = v[i] * slope_four[f, r + i].astype(F32)
            put(back, f, r + i, masked(x, r + i, 1, rows + 2, masks))

    conv(backward.at[3], seed, frames, rows + 2, fourth)

    def fifth(f, r, v):
        for i in range(2):
            back_three[f, r + i] = (v[i] * slope_three[f, r + i].astype(F32)).astype(BF16)

    conv(backward.at[2], back, frames, rows, fifth)
    if decode:
        buf, sems = refs[22:]
        for copy in decode_into(forward.at[3], four, frames, rows, buf, side, base, sems):
            copy.wait()


def decode_body(base, one, two, forward, whole, out, *scratch):
    four, (buf, sems) = scratch[:3], scratch[3:]
    rows = one.shape[1] - 2
    for f, ref in enumerate((one, two)):
        fill(four, f, ref, 0, rows + 2)
    for copy in decode_into(forward.at[3], four, 2, rows, buf, out, base, sems):
        copy.wait()


def unmix_body(outside, spots, *refs):
    picked = list(zip(refs, spots))
    backs, slopes = picked[:4], picked[4:]
    unmix, back_two, near, far = refs[6:]
    rows, chan = back_two.shape[1:3]
    weights = unmix[...]
    if outside:
        known = edge_masks("tm")[1]
        cut = (4 - outside) * chan
        end = (weights[:, cut:].astype(F32) * known).astype(BF16)
        weights = jnp.concatenate([weights[:, :cut], end], axis=1)
    for at in range(0, rows, WIDE):
        rhs = jnp.concatenate(
            [jnp.concatenate([ref[f, at + j] for ref, f in backs], axis=0) for j in range(WIDE)], axis=1
        )
        total = jnp.dot(weights, rhs, preferred_element_type=F32)
        width = total.shape[1] // WIDE
        for j in range(WIDE):
            r = at + j
            for i in range(2):
                x = total[i * chan : (i + 1) * chan, j * width : (j + 1) * width]
                slope, f = slopes[i]
                value = (x * slope[f, r].astype(F32)).astype(BF16)
                back_two[i, r] = value
    for i in range(2):
        take(back_two, i, 2, near, far, 2 * i)


def grad_body(base, spots, back_two, near, far, *refs):
    slopes, backward = list(zip(refs, spots)), refs[2]
    out, refs = refs[-9], refs[-8:]
    src, mid, (buf, sems) = refs[:3], refs[3:6], refs[6:]
    masks = edge_masks()
    frames, rows = back_two.shape[:2]
    for f in range(frames):
        fill(src, f, back_two, f, rows, *halos(near, far, 2 * f, 2, masks))

    def first(f, r, v):
        for i in range(2):
            slope, g = slopes[f]
            x = v[i] * slope[g, r + i].astype(F32)
            put(mid, f, r + i, masked(x, r + i, 1, rows + 2, masks))

    conv(backward.at[1], src, frames, rows + 2, first)
    for copy in decode_into(backward.at[0], mid, frames, rows, buf, out, base, sems):
        copy.wait()


def per_device(frames_in, conv_one, conv_two, temporal, conv_three, conv_four, cotangent):
    count, rows, chan, width = frames_in.shape
    unit = rows * chan * chan * width * 2 * 9 * 2

    def arr(*lead, dtype=BF16):
        return jax.ShapeDtypeStruct(tuple(lead) + (chan, width), dtype)

    def vm(*lead, dtype=BF16):
        return pltpu.VMEM(tuple(lead) + (chan, width), dtype)

    sems = pltpu.SemaphoreType.DMA((2, rows // 4))

    half = count - 2
    late_edges, edges = 4 * 2, 4 * half + 2 * count

    near, far = call(
        functools.partial(pack_late_body, half), (frames_in,), [VMEM],
        [arr(late_edges)] * 2, [VMEM] * 2,
    )
    near_late, far_late = exchanged(near, far)
    near, far = call(
        functools.partial(pack_body, half), (frames_in, cotangent), [VMEM] * 2,
        [arr(edges)] * 2, [VMEM] * 2,
    )
    near, far = exchanged(near, far)
    kernels = [jnp.transpose(k, (1, 2, 0, 3)) for k in (conv_one, conv_two, conv_three, conv_four)]
    two, four = 2 * chan, 4 * chan
    forward, backward, mix, unmix = call(
        prep_body, (*kernels, temporal), [VMEM] * 5,
        [jax.ShapeDtypeStruct((4, two, 3 * four), BF16)] * 2
        + [jax.ShapeDtypeStruct((two, four), BF16)] * 2,
        [VMEM] * 4, flops=unit // 4,
    )

    def encode(base, n, at, near, far):
        return call(
            functools.partial(encode_body, base, at), (frames_in, near, far, forward), [VMEM] * 4,
            [arr(n, rows + 4), arr(n, rows + 2), arr(n, rows)], [VMEM] * 3,
            [vm(n, rows + 8)] * 3 + [vm(n, rows + 6)] * 3, flops=3 * unit * n // 2,
        )

    def middle(base, n, acts, outside):
        decode = len(acts) == 4
        acts, spots = zip(*acts)
        side = arr(count, rows) if decode else arr(n, rows + 2)
        scratch = [vm(n, rows + 4)] * 3 + [vm(n, rows + 2)] * 3 + [vm(n, rows + 4)] * 3
        scratch += [vm(n, rows + 2)] * 3 + [vm(n, rows), vm(n, rows + 2)]
        if decode:
            scratch += [vm(n, rows), sems]
        return call(
            functools.partial(middle_body, base, outside, decode, spots),
            acts + (cotangent, near, far, forward, backward, mix),
            [VMEM] * (len(acts) + 6), [arr(n, rows), side], [VMEM, ANY if decode else VMEM], scratch,
            flops=5 * unit * n // 2,
        )

    def unmixed(backs, slopes, outside):
        ins, spots = zip(*(backs + slopes))
        return call(
            functools.partial(unmix_body, outside, spots), ins + (unmix,), [VMEM] * 7,
            [arr(2, rows), arr(4), arr(4)], [VMEM] * 3, flops=unit // 3,
        )

    def grad(base, back_two, near, far, slopes, whole):
        slopes, spots = zip(*slopes)
        ins, specs = (back_two, near, far) + slopes + (backward,), [VMEM] * 6
        if whole is not None:
            ins, specs = ins + (whole,), specs + [ANY]
        return call(
            functools.partial(grad_body, base, spots), ins, specs, arr(count, rows, dtype=F32), ANY,
            [vm(2, rows + 4)] * 3 + [vm(2, rows + 2)] * 3 + [vm(2, rows, dtype=F32), sems],
            {} if whole is None else {6: 0}, flops=2 * unit,
        )

    act_3, slope_one_3, slope_two_3 = encode(half + 1, 1, 4, near_late, far_late)
    before_1 = passed_along(act_3, "tm", 1)
    act_2, slope_one_2, slope_two_2 = encode(half, 1, 0, near_late, far_late)
    before_2 = passed_along(act_2, "tm", 1)
    act, slope_one, slope_two = encode(0, half, 0, near, far)
    back_late, decoded = middle(half, 2, [(act, 0), (act, 1), (act_2, 0), (act_3, 0)], 0)
    before_1, back_late = lax.optimization_barrier((before_1, back_late))
    back_1, act_four_1 = middle(1, 1, [(before_1, 0), (act, 0), (act, 1)], 1)
    after_1 = passed_along(back_1, "tm", -1)
    before_2, back_1 = lax.optimization_barrier((before_2, back_1))
    back_0, act_four_0 = middle(0, 1, [(before_2, 0), (before_1, 0), (act, 0)], 2)
    after_0 = passed_along(back_0, "tm", -1)
    backs = [(back_0, 0), (back_1, 0), (back_late, 0), (back_late, 1), (after_0, 0), (after_1, 0)]
    early, near, far = unmixed(backs[:4], [(slope_two, 0), (slope_two, 1)], 0)
    early_near, early_far = exchanged(near, far)
    late, near, far = unmixed(backs[2:], [(slope_two_2, 0), (slope_two_3, 0)], 2)
    late_near, late_far = exchanged(near, far)
    decoded = call(
        functools.partial(decode_body, 0), (act_four_0, act_four_1, forward, decoded), [VMEM] * 3 + [ANY],
        arr(count, rows), ANY, [vm(2, rows + 2)] * 3 + [vm(2, rows), sems], {3: 0},
        flops=unit,
    )
    grad_in = grad(0, early, early_near, early_far, [(slope_one, 0), (slope_one, 1)], None)
    grad_in = grad(half, late, late_near, late_far, [(slope_one_2, 0), (slope_one_3, 0)], grad_in)
    return decoded, grad_in


def solution(mesh):
    split = P("tm", "rows", None, None)
    return jax.shard_map(
        per_device,
        mesh=mesh,
        in_specs=(split, P(), P(), P(), P(), P(), split),
        out_specs=(split, split),
        check_vma=False,
    )
```
